32 devices in a mesh: grp: 2 (over y), row: 16 (over z, x, core).
Axes of the slice: x: 2, y: 2, z: 4, core: 2. Of those that a mesh axis runs over, the one named last changes fastest.
Arguments:
- diag_blocks: float32 [8192, 512], P('row'), may hold values from -0.6 to 2.6
- lower_coupling: float32 [8192, 64], P('row'), may hold values from -0.3125 to 0.3125
- upper_coupling: float32 [8192, 64], P('row'), may hold values from -0.3125 to 0.3125
- right_sides: float32 [8192, 1024], P('row', 'grp'), parts along dimension 1, may hold values from -108 to 108
Outputs:
- solution: float32 [8192, 1024], P('row', 'grp'), parts along dimension 1
- res_norms: float32 [8, 1024], P(None, 'grp'), parts along dimension 1
The draws below stay inside these ranges and needn't reach their ends.
There are 2 independent parts, one for each index of `grp`. The reference program is written for one: setup_inputs(seed, part) draws one part's arguments, and reference() takes and returns one part's arrays. A program takes and returns all parts, laid end to end along the dimension named above; an argument that names none is the same for every part. Nothing has to cross between parts.
All inputs are finite; a program needn't handle non-finite values.
Results may differ from the reference program's by a relative error of at most 0.0001.
Values sent between devices are 32-bit elements; how exact they have to be, the bound alone decides.
A program may use at most 64 MiB of HBM per device.

```python
import math
import jax
import jax.numpy as jnp
from jax import lax

B = 512
W = 64
C = 512
SWEEPS = 8
N = 8192
N_ROW = 16


def draw_diag_blocks(key, part):
    first, second = jax.random.split(jax.random.fold_in(key, 31), 2)
    noise = jnp.clip(jax.random.normal(first, (N, B), jnp.float32), -4.0, 4.0)
    noise = noise * (0.8 / math.sqrt(B))
    pivots = jax.random.uniform(second, (N, 1), jnp.float32, 1.0, 2.0)
    local_rows = (jnp.arange(N, dtype=jnp.int32) % B)[:, None]
    columns = jnp.arange(B, dtype=jnp.int32)[None, :]
    marker = (local_rows == columns).astype(jnp.float32)
    return (noise + marker * pivots).astype(jnp.float32)


def draw_right_sides(key, part):
    first, second, third = jax.random.split(jax.random.fold_in(key, 47), 3)
    base = jnp.clip(jax.random.normal(first, (N, C), jnp.float32), -4.0, 4.0)
    trend = jnp.exp(math.log(3.0) * jnp.arange(N, dtype=jnp.float32) / N)[:, None]
    row_scale = jnp.exp(jax.random.uniform(second, (N, 1), jnp.float32, math.log(0.3), math.log(3.0)))
    col_scale = jnp.exp(jax.random.uniform(third, (1, C), jnp.float32, math.log(0.3), math.log(3.0)))
    return (base * trend * row_scale * col_scale).astype(jnp.float32)


def block_levels(key, shape, shards, least, largest):
    gain = 1.0
    for position, parts in shards:
        draws = jax.random.uniform(jax.random.fold_in(jax.random.fold_in(key, 6), position), (parts,), jnp.float32, least / len(shards), largest / len(shards))
        gain = gain * jnp.repeat(jnp.exp(draws), shape[position] // parts).reshape((-1,) + (1,) * (len(shape) - 1 - position))
    return gain


def bell_draw(rng, extent, spread, most, shards=(), held_as=jnp.bfloat16):
    drawn = jax.random.normal(rng, extent, jnp.float32) * spread
    if len(shards) > 0:
        drawn = block_levels(rng, extent, shards, -0.22, 0.18) * drawn
    return jnp.clip(drawn, min=-most, max=most).astype(held_as)


def setup_inputs(seed: int = 0, part: int = 0) -> dict:
    seeds = jax.random.split(jax.random.key(seed), 5)
    part_keys = jax.random.split(jax.random.fold_in(seeds[4], part), 5)
    diag_blocks = draw_diag_blocks(jax.random.fold_in(seeds[4], 71), part)
    lower_coupling = bell_draw(seeds[1], (N, W), (6 * W) ** -0.5, 0.3125, ((0, 16),), jnp.float32)
    upper_coupling = bell_draw(seeds[2], (N, W), (6 * W) ** -0.5, 0.3125, ((0, 16),), jnp.float32)
    right_sides = draw_right_sides(jax.random.fold_in(jax.random.fold_in(seeds[4], part), 71), part)
    return dict(diag_blocks=diag_blocks, lower_coupling=lower_coupling, upper_coupling=upper_coupling, right_sides=right_sides)


def reference(diag_blocks, lower_coupling, upper_coupling, right_sides):
    blocks = diag_blocks.reshape(N_ROW, B, B)
    lower_blocks = lower_coupling.reshape(N_ROW, B, W)
    upper_blocks = upper_coupling.reshape(N_ROW, B, W)
    sources = right_sides.reshape(N_ROW, B, C)
    pivots = jnp.diagonal(blocks, axis1=1, axis2=2)[:, :, None]
    solution = jnp.zeros((N_ROW, B, C), jnp.float32)
    norm_list = []
    for sweep_index in range(SWEEPS):
        before_rims = jnp.concatenate([jnp.zeros((1, W, C), jnp.float32), solution[:-1, B - W:]], 0)
        after_rims = jnp.concatenate([solution[1:, :W], jnp.zeros((1, W, C), jnp.float32)], 0)
        images = jnp.einsum('kij,kjc->kic', blocks, solution, precision=lax.Precision.HIGHEST)
        images = images + jnp.einsum('kiw,kwc->kic', lower_blocks, before_rims, precision=lax.Precision.HIGHEST)
        images = images + jnp.einsum('kiw,kwc->kic', upper_blocks, after_rims, precision=lax.Precision.HIGHEST)
        residual = sources - images
        norm_list.append(jnp.sqrt(lax.optimization_barrier(jnp.sum(residual * residual, axis=(0, 1)))))
        solution = solution + residual / pivots
    return (solution.reshape(N_ROW * B, C), jnp.stack(norm_list))
```

```python
import functools

import jax
import jax.numpy as jnp
from jax import lax
from jax.experimental import pallas as pl
from jax.experimental.pallas import tpu as pltpu
from jax.sharding import PartitionSpec as P

SWEEPS = 8
LANES = 128
GROUP = 256
STEP = 64


def split(value):
    high = value.astype(jnp.bfloat16)
    low = (value - high.astype(jnp.float32)).astype(jnp.bfloat16)
    return high, low


def dot(left, right):
    return jnp.dot(left, right, preferred_element_type=jnp.float32)


def halves(count):
    return pl.ds(0, count // 2), pl.ds(count // 2, count // 2)


def wide(column, size):
    return column if size == LANES else jnp.concatenate([column] * (size // LANES), axis=1)


def kernel(
    n, d_hbm, l_hbm, u_hbm, b_hbm, x_out, norm_out,
    dv, lu, xs, a_hi, a_lo, cf, c3, cx, w3, inv, acc, hi, lo, halo, own, pre, zs,
    send, recv, gsend, grecv, part, nears, fars, lates, load_sem, send_sem, recv_sem, gsem, psend, precv,
):
    me = lax.axis_index("row")
    rows, cols = xs.shape
    width = lu.shape[1]
    size = hi.shape[1]
    groups = cols // size
    last = rows - width
    chunks = rows // LANES
    core = lax.rem(me, 2)
    fast_row, slow_row = me + 1 - 2 * core, me - 1 + 2 * core
    has = jnp.logical_and(slow_row >= 0, slow_row < n)
    SLOW, FAST = 0, 1
    slow_rows = pl.ds(pl.multiple_of(core * last, width), width)
    fast_rows = pl.ds(pl.multiple_of((1 - core) * last, width), width)
    rest_rows = [pl.ds(pl.multiple_of(core * width + k * width, width), width) for k in range(last // width)]
    middle = pl.ds(width, last - width)

    order = [core * (chunks - 1), (1 - core) * (chunks - 1)] + list(range(1, chunks - 1))

    def chunk(m):
        return pl.ds(pl.multiple_of(m * LANES, LANES), LANES)

    def load(src, dst, k):
        return pltpu.make_async_copy(src, dst, load_sem.at[k])

    d_loads = [load(d_hbm.at[chunk(m)], dv.at[chunk(m)], k) for k, m in enumerate(order)]
    b_loads = [load(b_hbm.at[r], xs.at[r], chunks + k) for k, r in enumerate((slow_rows, fast_rows, middle))]
    c_loads = [load(l_hbm, lu.at[core], chunks + 3), load(u_hbm, lu.at[1 - core], chunks + 4)]
    for copy in (d_loads[0], b_loads[0], d_loads[1], b_loads[1], *c_loads, *d_loads[2:], b_loads[2]):
        copy.start()

    barrier = pltpu.get_barrier_semaphore()

    def greet(o, carry):
        pl.semaphore_signal(barrier, inc=1, device_id={"row": lax.rem(me + o, n)})
        return carry

    lax.fori_loop(1, n, greet, 0)

    @pl.when(jnp.logical_not(has))
    def _():
        recv[:, SLOW] = jnp.zeros_like(recv[:, SLOW])
        grecv[...] = jnp.zeros_like(grecv)

    def copy(s, side, g):
        return pltpu.make_async_remote_copy(
            src_ref=send.at[s, side, g], dst_ref=recv.at[s, side, g],
            send_sem=send_sem.at[s, side, g], recv_sem=recv_sem.at[s, side, g],
            device_id={"row": slow_row if side == SLOW else fast_row})

    reflect = pltpu.make_async_remote_copy(
        src_ref=gsend, dst_ref=grecv, send_sem=gsem.at[0], recv_sem=gsem.at[1],
        device_id={"row": slow_row})

    def ship(s, side, g):
        if side == FAST:
            copy(s, side, g).start()
        else:
            @pl.when(has)
            def _():
                copy(s, side, g).start()

    def span(g):
        return slice(g * size, (g + 1) * size)

    def scale(r):
        return wide(inv[r], size)

    def stack(ref, pair, *index):
        for k, value in enumerate((pair[0], pair[1], pair[0])):
            ref[*index, k * width:(k + 1) * width] = value

    def triple(value):
        high, low = split(value)
        return jnp.concatenate([high, high, low], axis=1)

    def keep(r, at, g, s):
        d = r * scale(at)
        hi[at], lo[at] = split(d)
        return d, jnp.sum(r * r, axis=0, keepdims=True)

    def note(s, g, sums):
        per = size // LANES
        for j in range(per):
            part[s, g * per + j:g * per + j + 1] = sums[:, j * LANES:(j + 1) * LANES]

    def advance(g):
        for at in halves(rows):
            acc[g, at] = dot(a_hi[at], hi[...]) + dot(a_hi[at], lo[...]) + dot(a_lo[at], hi[...])

    def pivots(m):
        block = dv[chunk(m), chunk(m)]
        eye = (lax.broadcasted_iota(jnp.int32, block.shape, 0)
               == lax.broadcasted_iota(jnp.int32, block.shape, 1))
        pivot = jnp.sum(jnp.where(eye, block, 0.0), axis=1, keepdims=True)
        inv[chunk(m)] = jnp.broadcast_to(1.0 / pivot, block.shape)

    def spread(m):
        for k in range(0, LANES, 32):
            at = pl.ds(pl.multiple_of(m * LANES + k, 32), 32)
            block = dv[at]
            eye = (lax.broadcasted_iota(jnp.int32, block.shape, 0) + (m * LANES + k)
                   == lax.broadcasted_iota(jnp.int32, block.shape, 1))
            a_hi[at], a_lo[at] = split(jnp.where(eye, 0.0, -block))

    d_loads[0].wait()
    pivots(order[0])
    b_loads[0].wait()
    for g in range(groups):
        send[0, SLOW, g] = xs[slow_rows, span(g)] * scale(slow_rows)
    d_loads[1].wait()
    pivots(order[1])
    b_loads[1].wait()
    for g in range(groups):
        send[0, FAST, g] = xs[fast_rows, span(g)] * scale(fast_rows)
    pl.semaphore_wait(barrier, n - 1)
    for g in range(groups):
        ship(0, FAST, g)
    ship(0, SLOW, 0)

    for c_load in c_loads:
        c_load.wait()
    cf[...] = -jnp.concatenate([lu[0], lu[1]], axis=0).T
    reflected = cf[slow_rows, :width] * inv[slow_rows, :width]
    gsend[...] = jnp.concatenate([reflected[:width // 2], reflected[width // 2:]], axis=1)

    @pl.when(has)
    def _():
        reflect.start()
    for g in range(1, groups):
        ship(0, SLOW, g)

    c3[...] = jnp.concatenate([triple(cf[:, width:]), triple(cf[:, :width])], axis=1)
    cx[...] = triple(cf[slow_rows, width:])
    for m in order[:2]:
        spread(m)
    for k, m in enumerate(order[2:]):
        d_loads[2 + k].wait()
        pivots(m)
        spread(m)

    b_loads[2].wait()
    for g in range(groups):
        total = jnp.zeros((1, size), jnp.float32)
        for k in range(0, rows, STEP):
            at = pl.ds(k, STEP)
            d, sums = keep(xs[at, span(g)], at, g, 0)
            total = total + sums
            xs[at, span(g)] = d
        note(0, g, total)
        stack(own, (hi[slow_rows], lo[slow_rows]), g)
        pre[g] = jnp.zeros_like(pre[g])
        advance(g)

    def early(s, g):
        copy(s, FAST, g).wait_recv()
        stack(halo, split(recv[s, FAST, g]), g, 0)

    def early_send(s, g):
        z = acc[g, slow_rows] + dot(cx[...], halo[g, 0].reshape(3 * width, size))
        send[s + 1, SLOW, g] = z * scale(slow_rows)
        ship(s + 1, SLOW, g)

    def correct(s, g, final):
        @pl.when(has)
        def _():
            copy(s, SLOW, g).wait_recv()
        stack(halo, split(recv[s, SLOW, g] + pre[g]), g, 1)
        total = jnp.zeros((1, size), jnp.float32)
        for at in halves(rows):
            zs[at] = dot(c3[at], halo[g].reshape(6 * width, size))
        for at in (fast_rows, *rest_rows):
            r = acc[g, at] + zs[at]
            if final:
                x_out[at, span(g)] = xs[at, span(g)] + r * scale(at)
                total = total + jnp.sum(r * r, axis=0, keepdims=True)
                continue
            d, sums = keep(r, at, g, s + 1)
            total = total + sums
            if at is fast_rows:
                send[s + 1, FAST, g] = d
                ship(s + 1, FAST, g)
            xs[at, span(g)] += d
        note(s + 1, g, total)

    def reflection(g):
        pre[g] = dot(w3[...], own[g])
        stack(own, (hi[slow_rows], lo[slow_rows]), g)

    early(0, 0)
    early_send(0, 0)

    def body(s, carry):
        for g in range(groups):
            correct(s, g, False)
            ahead = (s, g + 1) if g + 1 < groups else (s + 1, 0)
            early(*ahead)
            if g + 1 < groups:
                early_send(*ahead)
            else:
                @pl.when(s < SWEEPS - 3)
                def _():
                    early_send(*ahead)
            advance(g)
            if g == 0:
                @pl.when(s == 0)
                def _():
                    @pl.when(has)
                    def _():
                        reflect.wait_recv()
                    gathered = grecv[...]
                    w3[...] = triple(jnp.concatenate([gathered[:, :width], gathered[:, width:]], axis=0))
            reflection(g)
        return carry

    inner = nears.shape[0]
    outer = n // inner
    seat, bench = lax.rem(me, inner), lax.div(me, inner)
    done = SWEEPS - 1

    def near(o):
        return pltpu.make_async_remote_copy(
            src_ref=part.at[:done], dst_ref=nears.at[seat],
            send_sem=psend.at[0, o], recv_sem=precv.at[0, o],
            device_id={"row": bench * inner + lax.rem(seat + o, inner)})

    def far(o):
        return pltpu.make_async_remote_copy(
            src_ref=fars.at[bench], dst_ref=fars.at[bench],
            send_sem=psend.at[1, o], recv_sem=precv.at[1, o],
            device_id={"row": lax.rem(bench + o, outer) * inner + seat})

    def late(o):
        return pltpu.make_async_remote_copy(
            src_ref=part.at[done], dst_ref=lates.at[me],
            send_sem=psend.at[2, o], recv_sem=precv.at[2, o],
            device_id={"row": lax.rem(me + o, n)})

    def over(count, action):
        def one(o, carry):
            action(o)
            return carry

        lax.fori_loop(1, count, one, 0)

    lax.fori_loop(0, SWEEPS - 2, body, 0)
    over(inner, lambda o: near(o).start())
    nears[seat] = part[:done]
    for g in range(groups):
        correct(SWEEPS - 2, g, True)
        if g + 1 < groups:
            early(SWEEPS - 2, g + 1)
        if g == 0:
            over(inner, lambda o: near(o).wait_recv())
            sums = nears[0]
            for j in range(1, inner):
                sums = sums + nears[j]
            fars[bench] = sums
            over(outer, lambda o: far(o).start())
    over(n, lambda o: late(o).start())
    lates[me] = part[done]

    def drain(s, carry):
        for g in range(groups):
            copy(s, FAST, g).wait_send()

            @pl.when(has)
            def _():
                copy(s, SLOW, g).wait_send()
        return carry

    lax.fori_loop(0, SWEEPS - 1, drain, 0)

    @pl.when(has)
    def _():
        reflect.wait_send()
    over(inner, lambda o: near(o).wait_send())
    over(outer, lambda o: far(o).wait_recv())
    norms = fars[0]
    for j in range(1, outer):
        norms = norms + fars[j]
    norms = jnp.sqrt(norms)
    parts = cols // LANES
    for s in range(done):
        for g in range(parts):
            norm_out[s:s + 1, g * LANES:(g + 1) * LANES] = norms[s, g:g + 1]
    over(n, lambda o: late(o).wait_recv())
    norm = jnp.sqrt(lax.fori_loop(1, n, lambda j, t: t + lates[j], lates[0]))
    for g in range(parts):
        norm_out[done:, g * LANES:(g + 1) * LANES] = norm[g:g + 1]
    over(outer, lambda o: far(o).wait_send())
    over(n, lambda o: late(o).wait_send())


def local(n, diag_blocks, lower_coupling, upper_coupling, right_sides):
    rows, cols = right_sides.shape
    width = lower_coupling.shape[1]
    size = GROUP
    groups, parts = cols // size, cols // LANES
    inner = max(a for a in range(1, n + 1) if n % a == 0 and a * a <= n)
    f32, bf16 = jnp.float32, jnp.bfloat16
    return pl.pallas_call(
        functools.partial(kernel, n),
        out_shape=(pltpu.VMEM((rows, cols), f32), pltpu.VMEM((SWEEPS, cols), f32)),
        in_specs=[pl.BlockSpec(memory_space=pltpu.HBM)] * 4,
        out_specs=[pl.BlockSpec(memory_space=pltpu.VMEM)] * 2,
        scratch_shapes=[
            pltpu.VMEM((rows, rows), f32),
            pltpu.VMEM((2, width, rows), f32),
            pltpu.VMEM((rows, cols), f32),
            pltpu.VMEM((rows, rows), bf16),
            pltpu.VMEM((rows, rows), bf16),
            pltpu.VMEM((rows, 2 * width), f32),
            pltpu.VMEM((rows, 6 * width), bf16),
            pltpu.VMEM((width, 3 * width), bf16),
            pltpu.VMEM((width, 3 * width), bf16),
            pltpu.VMEM((rows, LANES), f32),
            pltpu.VMEM((groups, rows, size), f32),
            pltpu.VMEM((rows, size), bf16),
            pltpu.VMEM((rows, size), bf16),
            pltpu.VMEM((groups, 2, 3 * width, size), bf16),
            pltpu.VMEM((groups, 3 * width, size), bf16),
            pltpu.VMEM((groups, width, size), f32),
            pltpu.VMEM((rows, size), f32),
            pltpu.VMEM((SWEEPS - 1, 2, groups, width, size), f32),
            pltpu.VMEM((SWEEPS - 1, 2, groups, width, size), f32),
            pltpu.VMEM((width // 2, 2 * width), f32),
            pltpu.VMEM((width // 2, 2 * width), f32),
            pltpu.VMEM((SWEEPS, parts, LANES), f32),
            pltpu.VMEM((inner, SWEEPS - 1, parts, LANES), f32),
            pltpu.VMEM((n // inner, SWEEPS - 1, parts, LANES), f32),
            pltpu.VMEM((n, parts, LANES), f32),
            pltpu.SemaphoreType.DMA((rows // LANES + 5,)),
            pltpu.SemaphoreType.DMA((SWEEPS - 1, 2, groups)),
            pltpu.SemaphoreType.DMA((SWEEPS - 1, 2, groups)),
            pltpu.SemaphoreType.DMA((2,)),
            pltpu.SemaphoreType.DMA((3, n)),
            pltpu.SemaphoreType.DMA((3, n)),
        ],
        compiler_params=pltpu.CompilerParams(
            collective_id=0, has_side_effects=True, vmem_limit_bytes=62 * 2**20),
    )(diag_blocks, lower_coupling.T, upper_coupling.T, right_sides)


def solution(mesh):
    return jax.shard_map(
        functools.partial(local, mesh.shape["row"]),
        mesh=mesh,
        in_specs=(P("row", None), P("row", None), P("row", None), P("row", "grp")),
        out_specs=(P("row", "grp"), P(None, "grp")),
        check_vma=False,
    )
```

```python
import functools

import jax
import jax.numpy as jnp
from jax import lax
from jax.experimental import pallas as pl
from jax.experimental.pallas import tpu as pltpu
from jax.sharding import PartitionSpec as P

SWEEPS = 8
LANES = 128
GROUP = 256
STEP = 64
PAUSE = 3


def split(value):
    high = value.astype(jnp.bfloat16)
    low = (value - high.astype(jnp.float32)).astype(jnp.bfloat16)
    return high, low


def dot(left, right):
    return jnp.dot(left, right, preferred_element_type=jnp.float32)


def halves(count):
    return pl.ds(0, count // 2), pl.ds(count // 2, count // 2)


def wide(column, size):
    return column if size == LANES else jnp.concatenate([column] * (size // LANES), axis=1)


def kernel(
    n, d_hbm, l_hbm, u_hbm, b_hbm, x_out, norm_out,
    dv, lu, xs, a_hi, a_lo, cf, c3, cx, w3, inv, acc, hi, lo, halo, own, pre, zs,
    send, recv, gsend, grecv, part, nears, fars, lates, load_sem, send_sem, recv_sem, gsem, psend, precv, lsem, waves,
):
    me = lax.axis_index("row")
    rows, cols = xs.shape
    width = lu.shape[1]
    size = hi.shape[1]
    groups = cols // size
    last = rows - width
    chunks = rows // LANES
    core = lax.rem(me, 2)
    fast_row, slow_row = me + 1 - 2 * core, me - 1 + 2 * core
    has = jnp.logical_and(slow_row >= 0, slow_row < n)
    SLOW, FAST = 0, 1
    slow_rows = pl.ds(pl.multiple_of(core * last, width), width)
    fast_rows = pl.ds(pl.multiple_of((1 - core) * last, width), width)
    rest_rows = [pl.ds(pl.multiple_of(core * width + k * width, width), width) for k in range(last // width)]
    middle = pl.ds(width, last - width)

    order = [core * (chunks - 1), (1 - core) * (chunks - 1)] + list(range(1, chunks - 1))

    def chunk(m):
        return pl.ds(pl.multiple_of(m * LANES, LANES), LANES)

    def load(src, dst, k):
        return pltpu.make_async_copy(src, dst, load_sem.at[k])

    d_loads = [load(d_hbm.at[chunk(m)], dv.at[chunk(m)], k) for k, m in enumerate(order)]
    b_loads = [load(b_hbm.at[r], xs.at[r], chunks + k) for k, r in enumerate((slow_rows, fast_rows, middle))]
    c_loads = [load(l_hbm, lu.at[core], chunks + 3), load(u_hbm, lu.at[1 - core], chunks + 4)]
    edge = pl.ds(pl.multiple_of(core * (rows - LANES), LANES), LANES)
    for copy in (d_loads[0], b_loads[0], *c_loads, d_loads[1], b_loads[1], *d_loads[2:], b_loads[2]):
        copy.start()

    barrier = pltpu.get_barrier_semaphore()

    pl.semaphore_signal(barrier, inc=1, device_id={"row": fast_row})

    @pl.when(has)
    def _():
        pl.semaphore_signal(barrier, inc=1, device_id={"row": slow_row})

    reach = SWEEPS // 2
    hops = [reach << k for k in range(n) if reach << k < n]

    def wave(k):
        for far_row in (me - hops[k], me + hops[k]):
            @pl.when(jnp.logical_and(far_row >= 0, far_row < n))
            def _():
                pl.semaphore_signal(waves.at[k], inc=1, device_id={"row": far_row})

    def await_wave(k):
        pl.semaphore_wait(waves.at[k], (me >= hops[k]).astype(jnp.int32) + (me + hops[k] < n).astype(jnp.int32))

    @pl.when(jnp.logical_not(has))
    def _():
        recv[:, SLOW] = jnp.zeros_like(recv[:, SLOW])
        grecv[...] = jnp.zeros_like(grecv)

    def copy(s, side, g):
        return pltpu.make_async_remote_copy(
            src_ref=send.at[s, side, g], dst_ref=recv.at[s, side, g],
            send_sem=send_sem.at[s, side, g], recv_sem=recv_sem.at[s, side, g],
            device_id={"row": slow_row if side == SLOW else fast_row})

    reflect = pltpu.make_async_remote_copy(
        src_ref=gsend, dst_ref=grecv, send_sem=gsem.at[0], recv_sem=gsem.at[1],
        device_id={"row": slow_row})

    def ship(s, side, g):
        if side == FAST:
            copy(s, side, g).start()
        else:
            @pl.when(has)
            def _():
                copy(s, side, g).start()

    def span(g):
        return slice(g * size, (g + 1) * size)

    def scale(r):
        return wide(inv[r], size)

    def stack(ref, pair, *index):
        for k, value in enumerate((pair[0], pair[1], pair[0])):
            ref[*index, k * width:(k + 1) * width] = value

    def triple(value):
        high, low = split(value)
        return jnp.concatenate([high, high, low], axis=1)

    def keep(r, at, g, s):
        d = r * scale(at)
        hi[at], lo[at] = split(d)
        return d, jnp.sum(r * r, axis=0, keepdims=True)

    def note(s, g, sums):
        per = size // LANES
        for j in range(per):
            part[s, g * per + j:g * per + j + 1] = sums[:, j * LANES:(j + 1) * LANES]

    def advance(g):
        for at in halves(rows):
            total = jnp.zeros((rows // 2, size), jnp.float32)
            for k in halves(rows):
                total = total + (dot(a_hi[at, k], hi[k]) + dot(a_hi[at, k], lo[k]) + dot(a_lo[at, k], hi[k]))
            acc[g, at] = total

    def pivots(m):
        block = dv[chunk(m), chunk(m)]
        eye = (lax.broadcasted_iota(jnp.int32, block.shape, 0)
               == lax.broadcasted_iota(jnp.int32, block.shape, 1))
        pivot = jnp.sum(jnp.where(eye, block, 0.0), axis=1, keepdims=True)
        inv[chunk(m)] = jnp.broadcast_to(1.0 / pivot, block.shape)

    def spread(m):
        for k in range(0, LANES, 32):
            at = pl.ds(pl.multiple_of(m * LANES + k, 32), 32)
            block = dv[at]
            eye = (lax.broadcasted_iota(jnp.int32, block.shape, 0) + (m * LANES + k)
                   == lax.broadcasted_iota(jnp.int32, block.shape, 1))
            a_hi[at], a_lo[at] = split(jnp.where(eye, 0.0, -block))

    d_loads[0].wait()
    pivots(order[0])
    b_loads[0].wait()
    for g in range(groups):
        send[0, SLOW, g] = xs[slow_rows, span(g)] * scale(slow_rows)
    for c_load in c_loads:
        c_load.wait()
    cf[edge] = -jnp.concatenate([lu[0, :, edge], lu[1, :, edge]], axis=0).T
    reflected = cf[slow_rows, :width] * inv[slow_rows, :width]
    gsend[...] = jnp.concatenate([reflected[:width // 2], reflected[width // 2:]], axis=1)
    pl.semaphore_wait(barrier, 1 + has.astype(jnp.int32))
    ship(0, SLOW, 0)
    d_loads[1].wait()
    pivots(order[1])
    b_loads[1].wait()
    for g in range(groups):
        send[0, FAST, g] = xs[fast_rows, span(g)] * scale(fast_rows)
        ship(0, FAST, g)

    cf[...] = -jnp.concatenate([lu[0], lu[1]], axis=0).T
    c3[...] = jnp.concatenate([triple(cf[:, width:]), triple(cf[:, :width])], axis=1)
    cx[...] = triple(cf[slow_rows, width:])
    for m in order[:2]:
        spread(m)
    for k, m in enumerate(order[2:]):
        d_loads[2 + k].wait()
        pivots(m)
        spread(m)

    b_loads[2].wait()
    for g in range(groups):
        total = jnp.zeros((1, size), jnp.float32)
        for k in range(0, rows, STEP):
            at = pl.ds(k, STEP)
            d, sums = keep(xs[at, span(g)], at, g, 0)
            total = total + sums
            xs[at, span(g)] = d
        note(0, g, total)
        stack(own, (hi[slow_rows], lo[slow_rows]), g, 0)
        pre[g] = jnp.zeros_like(pre[g])
        advance(g)
        if g + 1 < groups:
            ship(0, SLOW, g + 1)

    @pl.when(has)
    def _():
        reflect.start()

    def share(g):
        return dot(cx[...], halo[g, 0].reshape(3 * width, size))

    def early(s, g, z):
        send[s + 1, SLOW, g] = (acc[g, slow_rows] + z) * scale(slow_rows)

        @pl.when(jnp.logical_and(has, s < SWEEPS - 2))
        def _():
            copy(s + 1, SLOW, g).start()

    def take_fast(s, g):
        copy(s, FAST, g).wait_recv()
        stack(halo, split(recv[s, FAST, g]), g, 0)

    def take_slow(s, g):
        @pl.when(has)
        def _():
            copy(s, SLOW, g).wait_recv()
        stack(halo, split(recv[s, SLOW, g] + pre[g]), g, 1)

    def correct(s, g, final, between=lambda: None):
        total = jnp.zeros((1, size), jnp.float32)
        for k, at in enumerate((fast_rows, *rest_rows)):
            if k == PAUSE:
                between()
            r = acc[g, at] + zs[at]
            if final:
                x_out[at, span(g)] = xs[at, span(g)] + r * scale(at)
                total = total + jnp.sum(r * r, axis=0, keepdims=True)
                continue
            d, sums = keep(r, at, g, s + 1)
            total = total + sums
            if at is fast_rows:
                send[s + 1, FAST, g] = d
                ship(s + 1, FAST, g)
            xs[at, span(g)] += d
        note(s + 1, g, total)

    def couple(g):
        for at in halves(rows):
            zs[at] = dot(c3[at], halo[g].reshape(6 * width, size))

    take_fast(0, 0)
    early(0, 0, share(0))

    inner = nears.shape[0]
    outer = n // inner
    seat, bench = lax.rem(me, inner), lax.div(me, inner)
    done = SWEEPS - 2

    def near(o):
        return pltpu.make_async_remote_copy(
            src_ref=part.at[:done], dst_ref=nears.at[seat],
            send_sem=psend.at[0, o], recv_sem=precv.at[0, o],
            device_id={"row": bench * inner + lax.rem(seat + o, inner)})

    def far(o):
        return pltpu.make_async_remote_copy(
            src_ref=fars.at[bench], dst_ref=fars.at[bench],
            send_sem=psend.at[1, o], recv_sem=precv.at[1, o],
            device_id={"row": lax.rem(bench + o, outer) * inner + seat})

    def late(o):
        return pltpu.make_async_remote_copy(
            src_ref=part.at[done:], dst_ref=lates.at[me],
            send_sem=lsem.at[0], recv_sem=lsem.at[1],
            device_id={"row": lax.rem(me + o, n)})

    def lates_all(k):
        return pltpu.make_async_copy(lates.at[1:], lates.at[1:], lsem.at[k])

    def over(count, action):
        def one(o, carry):
            action(o)
            return carry

        lax.fori_loop(1, count, one, 0)

    def step(s, g, known):
        ahead = (s, g + 1) if g + 1 < groups else (s + 1, 0)
        take_slow(s, g)
        take_fast(*ahead)
        z = share(ahead[1])
        couple(g)
        if known:
            pre[g] = dot(w3[...], own[g, 1])
        early(*ahead, z)
        correct(s, g, False)
        advance(g)
        stack(own, (hi[slow_rows], lo[slow_rows]), g, 1)

    for g in range(groups):
        step(0, g, False)

    @pl.when(has)
    def _():
        reflect.wait_recv()
    gathered = grecv[...]
    w3[...] = triple(jnp.concatenate([gathered[:, :width], gathered[:, width:]], axis=0))
    for g in range(groups):
        pre[g] = dot(w3[...], own[g, 0])
    def body(s, carry):
        if hops:
            @pl.when(s == reach - 1)
            def _():
                wave(0)

        @pl.when(s == SWEEPS - 3)
        def _():
            if hops:
                await_wave(0)
            if len(hops) > 1:
                wave(1)
            over(inner, lambda o: near(o).start())
        for g in range(groups):
            step(s, g, True)
        return carry

    lax.fori_loop(1, SWEEPS - 2, body, 0)
    for k in range(1, len(hops)):
        await_wave(k)
        if k + 1 < len(hops):
            wave(k + 1)
    nears[seat] = part[:done]
    over(inner, lambda o: near(o).wait_recv())
    sums = nears[0]
    for j in range(1, inner):
        sums = sums + nears[j]
    fars[bench] = sums
    over(outer, lambda o: far(o).start())
    for g in range(groups):
        take_slow(SWEEPS - 2, g)
        if g + 1 < groups:
            take_fast(SWEEPS - 2, g + 1)
        couple(g)
        correct(SWEEPS - 2, g, True)
    over(n, lambda o: late(o).start())
    lates[me] = part[done:]

    def drain(s, carry):
        for g in range(groups):
            copy(s, FAST, g).wait_send()

            @pl.when(has)
            def _():
                copy(s, SLOW, g).wait_send()
        return carry

    lax.fori_loop(0, SWEEPS - 1, drain, 0)

    @pl.when(has)
    def _():
        reflect.wait_send()
    over(inner, lambda o: near(o).wait_send())
    over(outer, lambda o: far(o).wait_recv())
    parts = cols // LANES

    def finish(total, first):
        norms = jnp.sqrt(total)
        for s in range(total.shape[0]):
            for g in range(parts):
                norm_out[first + s:first + s + 1, g * LANES:(g + 1) * LANES] = norms[s, g:g + 1]

    finish(sum((fars[j] for j in range(1, outer)), fars[0]), 0)
    over(outer, lambda o: far(o).wait_send())
    lates_all(0).wait()
    lates_all(1).wait()
    terms = [lates[j] for j in range(n)]
    while len(terms) > 1:
        terms = [a + b for a, b in zip(terms[::2], terms[1::2])] + terms[len(terms) // 2 * 2:]
    finish(terms[0], done)


def local(n, diag_blocks, lower_coupling, upper_coupling, right_sides):
    rows, cols = right_sides.shape
    width = lower_coupling.shape[1]
    size = GROUP
    groups, parts = cols // size, cols // LANES
    inner = max(a for a in range(1, n + 1) if n % a == 0 and a * a <= n)
    f32, bf16 = jnp.float32, jnp.bfloat16
    return pl.pallas_call(
        functools.partial(kernel, n),
        out_shape=(pltpu.VMEM((rows, cols), f32), pltpu.VMEM((SWEEPS, cols), f32)),
        in_specs=[pl.BlockSpec(memory_space=pltpu.HBM)] * 4,
        out_specs=[pl.BlockSpec(memory_space=pltpu.VMEM)] * 2,
        scratch_shapes=[
            pltpu.VMEM((rows, rows), f32),
            pltpu.VMEM((2, width, rows), f32),
            pltpu.VMEM((rows, cols), f32),
            pltpu.VMEM((rows, rows), bf16),
            pltpu.VMEM((rows, rows), bf16),
            pltpu.VMEM((rows, 2 * width), f32),
            pltpu.VMEM((rows, 6 * width), bf16),
            pltpu.VMEM((width, 3 * width), bf16),
            pltpu.VMEM((width, 3 * width), bf16),
            pltpu.VMEM((rows, LANES), f32),
            pltpu.VMEM((groups, rows, size), f32),
            pltpu.VMEM((rows, size), bf16),
            pltpu.VMEM((rows, size), bf16),
            pltpu.VMEM((groups, 2, 3 * width, size), bf16),
            pltpu.VMEM((groups, 2, 3 * width, size), bf16),
            pltpu.VMEM((groups, width, size), f32),
            pltpu.VMEM((rows, size), f32),
            pltpu.VMEM((SWEEPS, 2, groups, width, size), f32),
            pltpu.VMEM((SWEEPS - 1, 2, groups, width, size), f32),
            pltpu.VMEM((width // 2, 2 * width), f32),
            pltpu.VMEM((width // 2, 2 * width), f32),
            pltpu.VMEM((SWEEPS, parts, LANES), f32),
            pltpu.VMEM((inner, SWEEPS - 2, parts, LANES), f32),
            pltpu.VMEM((n // inner, SWEEPS - 2, parts, LANES), f32),
            pltpu.VMEM((n, 2, parts, LANES), f32),
            pltpu.SemaphoreType.DMA((rows // LANES + 5,)),
            pltpu.SemaphoreType.DMA((SWEEPS - 1, 2, groups)),
            pltpu.SemaphoreType.DMA((SWEEPS - 1, 2, groups)),
            pltpu.SemaphoreType.DMA((2,)),
            pltpu.SemaphoreType.DMA((2, n)),
            pltpu.SemaphoreType.DMA((2, n)),
            pltpu.SemaphoreType.DMA((2,)),
            pltpu.SemaphoreType.REGULAR((max(n.bit_length() - 1, 1),)),
        ],
        compiler_params=pltpu.CompilerParams(
            collective_id=0, has_side_effects=True, vmem_limit_bytes=62 * 2**20),
    )(diag_blocks, lower_coupling.T, upper_coupling.T, right_sides)


def solution(mesh):
    return jax.shard_map(
        functools.partial(local, mesh.shape["row"]),
        mesh=mesh,
        in_specs=(P("row", None), P("row", None), P("row", None), P("row", "grp")),
        out_specs=(P("row", "grp"), P(None, "grp")),
        check_vma=False,
    )
```

```python
import functools

import jax
import jax.numpy as jnp
from jax import lax
from jax.experimental import pallas as pl
from jax.experimental.pallas import tpu as pltpu
from jax.sharding import PartitionSpec as P

SWEEPS = 8
LANES = 128
GROUP = 256
STEP = 64
PAUSE = 3


def split(value):
    high = value.astype(jnp.bfloat16)
    low = (value - high.astype(jnp.float32)).astype(jnp.bfloat16)
    return high, low


def dot(left, right):
    return jnp.dot(left, right, preferred_element_type=jnp.float32)


def reaches(n):
    return [hop for hop in (SWEEPS // 2 << k for k in range(n)) if hop < n]


def halves(count):
    return pl.ds(0, count // 2), pl.ds(count // 2, count // 2)


def wide(column, size):
    return column if size == LANES else jnp.concatenate([column] * (size // LANES), axis=1)


def kernel(
    n, d_hbm, l_hbm, u_hbm, b_hbm, x_out, norm_out,
    dv, lu, xs, a_hi, a_lo, cf, c3, cx, w3, inv, acc, hi, lo, halo, own, pre, zs,
    send, recv, gsend, grecv, part, nears, fars, lates, load_sem, send_sem, recv_sem, gsem, psend, precv, lsem, waves,
):
    me = lax.axis_index("row")
    rows, cols = xs.shape
    width = lu.shape[1]
    size = hi.shape[1]
    groups = cols // size
    last = rows - width
    chunks = rows // LANES
    core = lax.rem(me, 2)
    fast_row, slow_row = me + 1 - 2 * core, me - 1 + 2 * core
    has = jnp.logical_and(slow_row >= 0, slow_row < n)
    SLOW, FAST = 0, 1
    slow_rows = pl.ds(pl.multiple_of(core * last, width), width)
    fast_rows = pl.ds(pl.multiple_of((1 - core) * last, width), width)
    rest_rows = [pl.ds(pl.multiple_of(core * width + k * width, width), width) for k in range(last // width)]
    middle = pl.ds(width, last - width)

    order = [core * (chunks - 1), (1 - core) * (chunks - 1)] + list(range(1, chunks - 1))

    def chunk(m):
        return pl.ds(pl.multiple_of(m * LANES, LANES), LANES)

    def load(src, dst, k):
        return pltpu.make_async_copy(src, dst, load_sem.at[k])

    d_loads = [load(d_hbm.at[chunk(m)], dv.at[chunk(m)], k) for k, m in enumerate(order)]
    b_loads = [load(b_hbm.at[r], xs.at[r], chunks + k) for k, r in enumerate((slow_rows, fast_rows, middle))]
    c_loads = [load(l_hbm, lu.at[core], chunks + 3), load(u_hbm, lu.at[1 - core], chunks + 4)]
    edge = pl.ds(pl.multiple_of(core * (rows - LANES), LANES), LANES)
    for copy in (d_loads[0], b_loads[0], *c_loads, d_loads[1], b_loads[1], *d_loads[2:], b_loads[2]):
        copy.start()

    barrier = pltpu.get_barrier_semaphore()

    pl.semaphore_signal(barrier, inc=1, device_id={"row": fast_row})

    @pl.when(has)
    def _():
        pl.semaphore_signal(barrier, inc=1, device_id={"row": slow_row})

    hops = reaches(n)
    reach = SWEEPS // 2

    def wave(k):
        for far_row in (me - hops[k], me + hops[k]):
            @pl.when(jnp.logical_and(far_row >= 0, far_row < n))
            def _():
                pl.semaphore_signal(waves.at[k], inc=1, device_id={"row": far_row})

    def await_wave(k):
        pl.semaphore_wait(waves.at[k], (me >= hops[k]).astype(jnp.int32) + (me + hops[k] < n).astype(jnp.int32))

    @pl.when(jnp.logical_not(has))
    def _():
        recv[:, SLOW] = jnp.zeros_like(recv[:, SLOW])
        grecv[...] = jnp.zeros_like(grecv)

    def copy(s, side, g):
        return pltpu.make_async_remote_copy(
            src_ref=send.at[s, side, g], dst_ref=recv.at[s, side, g],
            send_sem=send_sem.at[side], recv_sem=recv_sem.at[s, side, g],
            device_id={"row": slow_row if side == SLOW else fast_row})

    reflect = pltpu.make_async_remote_copy(
        src_ref=gsend, dst_ref=grecv, send_sem=gsem.at[0], recv_sem=gsem.at[1],
        device_id={"row": slow_row})

    def ship(s, side, g):
        if side == FAST:
            copy(s, side, g).start()
        else:
            @pl.when(has)
            def _():
                copy(s, side, g).start()

    def span(g):
        return slice(g * size, (g + 1) * size)

    def scale(r):
        return wide(inv[r], size)

    def stack(ref, pair, *index):
        for k, value in enumerate((pair[0], pair[1], pair[0])):
            ref[*index, k * width:(k + 1) * width] = value

    def triple(value):
        high, low = split(value)
        return jnp.concatenate([high, high, low], axis=1)

    def keep(r, at, g, s):
        d = r * scale(at)
        hi[at], lo[at] = split(d)
        return d, jnp.sum(r * r, axis=0, keepdims=True)

    def note(s, g, sums):
        per = size // LANES
        for j in range(per):
            part[s, g * per + j:g * per + j + 1] = sums[:, j * LANES:(j + 1) * LANES]

    def advance(g):
        for at in halves(rows):
            total = jnp.zeros((rows // 2, size), jnp.float32)
            for k in halves(rows):
                total = total + (dot(a_hi[at, k], hi[k]) + dot(a_hi[at, k], lo[k]) + dot(a_lo[at, k], hi[k]))
            acc[g, at] = total

    def pivots(m):
        block = dv[chunk(m), chunk(m)]
        eye = (lax.broadcasted_iota(jnp.int32, block.shape, 0)
               == lax.broadcasted_iota(jnp.int32, block.shape, 1))
        pivot = jnp.sum(jnp.where(eye, block, 0.0), axis=1, keepdims=True)
        inv[chunk(m)] = jnp.broadcast_to(1.0 / pivot, block.shape)

    def spread(m):
        for k in range(0, LANES, 32):
            at = pl.ds(pl.multiple_of(m * LANES + k, 32), 32)
            block = dv[at]
            eye = (lax.broadcasted_iota(jnp.int32, block.shape, 0) + (m * LANES + k)
                   == lax.broadcasted_iota(jnp.int32, block.shape, 1))
            a_hi[at], a_lo[at] = split(jnp.where(eye, 0.0, -block))

    d_loads[0].wait()
    pivots(order[0])
    b_loads[0].wait()
    for g in range(groups):
        send[0, SLOW, g] = xs[slow_rows, span(g)] * scale(slow_rows)
    for c_load in c_loads:
        c_load.wait()
    cf[edge] = -jnp.concatenate([lu[0, :, edge], lu[1, :, edge]], axis=0).T
    reflected = cf[slow_rows, :width] * inv[slow_rows, :width]
    gsend[...] = jnp.concatenate([reflected[:width // 2], reflected[width // 2:]], axis=1)
    pl.semaphore_wait(barrier, 1 + has.astype(jnp.int32))
    ship(0, SLOW, 0)
    d_loads[1].wait()
    pivots(order[1])
    b_loads[1].wait()
    for g in range(groups):
        send[0, FAST, g] = xs[fast_rows, span(g)] * scale(fast_rows)
        ship(0, FAST, g)

    cf[...] = -jnp.concatenate([lu[0], lu[1]], axis=0).T
    c3[...] = jnp.concatenate([triple(cf[:, width:]), triple(cf[:, :width])], axis=1)
    cx[...] = triple(cf[slow_rows, width:])
    for m in order[:2]:
        spread(m)
    for k, m in enumerate(order[2:]):
        d_loads[2 + k].wait()
        pivots(m)
        spread(m)

    for g in range(1, groups):
        ship(0, SLOW, g)
    b_loads[2].wait()
    for g in range(groups):
        total = jnp.zeros((1, size), jnp.float32)
        for k in range(0, rows, STEP):
            at = pl.ds(k, STEP)
            d, sums = keep(xs[at, span(g)], at, g, 0)
            total = total + sums
            xs[at, span(g)] = d
        note(0, g, total)
        stack(own, (hi[slow_rows], lo[slow_rows]), g, 0)
        pre[g] = jnp.zeros_like(pre[g])
        advance(g)

    @pl.when(has)
    def _():
        reflect.start()

    def share(g):
        return dot(cx[...], halo[g, 0].reshape(3 * width, size))

    def early(s, g, z):
        send[s + 1, SLOW, g] = (acc[g, slow_rows] + z) * scale(slow_rows)

        @pl.when(jnp.logical_and(has, s < SWEEPS - 2))
        def _():
            copy(s + 1, SLOW, g).start()

    def take_fast(s, g):
        copy(s, FAST, g).wait_recv()
        stack(halo, split(recv[s, FAST, g]), g, 0)

    def take_slow(s, g):
        @pl.when(has)
        def _():
            copy(s, SLOW, g).wait_recv()
        stack(halo, split(recv[s, SLOW, g] + pre[g]), g, 1)

    def correct(s, g, final, between=lambda: None):
        total = jnp.zeros((1, size), jnp.float32)
        for k, at in enumerate((fast_rows, *rest_rows)):
            if k == PAUSE:
                between()
            r = acc[g, at] + zs[g, at]
            if final:
                total = total + jnp.sum(r * r, axis=0, keepdims=True)
                continue
            d, sums = keep(r, at, g, s + 1)
            total = total + sums
            if at is fast_rows:
                send[s + 1, FAST, g] = d
                ship(s + 1, FAST, g)
            xs[at, span(g)] += d
        note(s + 1, g, total)

    def couple(g):
        for at in halves(rows):
            zs[g, at] = dot(c3[at], halo[g].reshape(6 * width, size))

    take_fast(0, 0)
    early(0, 0, share(0))

    inner = nears.shape[0]
    outer = n // inner
    seat, bench = lax.rem(me, inner), lax.div(me, inner)
    done = SWEEPS - 2

    def near(o):
        return pltpu.make_async_remote_copy(
            src_ref=part.at[:done], dst_ref=nears.at[seat],
            send_sem=psend.at[0], recv_sem=precv.at[0],
            device_id={"row": bench * inner + lax.rem(seat + o, inner)})

    def far(o):
        return pltpu.make_async_remote_copy(
            src_ref=fars.at[bench], dst_ref=fars.at[bench],
            send_sem=psend.at[1], recv_sem=precv.at[1],
            device_id={"row": lax.rem(bench + o, outer) * inner + seat})

    def late(o):
        return pltpu.make_async_remote_copy(
            src_ref=part.at[done:], dst_ref=lates.at[me],
            send_sem=lsem.at[0], recv_sem=lsem.at[1],
            device_id={"row": lax.rem(me + o, n)})

    def lates_all(k):
        return pltpu.make_async_copy(lates.at[1:], lates.at[1:], lsem.at[k])

    def over(count, action):
        def one(o, carry):
            action(o)
            return carry

        lax.fori_loop(1, count, one, 0)

    def step(s, g, known):
        ahead = (s, g + 1) if g + 1 < groups else (s + 1, 0)
        take_slow(s, g)
        couple(g)
        take_fast(*ahead)
        z = share(ahead[1])
        if known:
            pre[g] = dot(w3[...], own[g, 1])
        early(*ahead, z)
        correct(s, g, False)
        advance(g)
        stack(own, (hi[slow_rows], lo[slow_rows]), g, 1)

    for g in range(groups):
        step(0, g, False)

    @pl.when(has)
    def _():
        reflect.wait_recv()
    gathered = grecv[...]
    w3[...] = triple(jnp.concatenate([gathered[:, :width], gathered[:, width:]], axis=0))
    for g in range(groups):
        pre[g] = dot(w3[...], own[g, 0])
    def body(s, carry):
        if hops:
            @pl.when(s == reach - 1)
            def _():
                wave(0)

        @pl.when(s == SWEEPS - 3)
        def _():
            if hops:
                await_wave(0)
            if len(hops) > 1:
                wave(1)
            over(inner, lambda o: near(o).start())
        for g in range(groups):
            step(s, g, True)
        return carry

    lax.fori_loop(1, SWEEPS - 2, body, 0)
    for k in range(1, len(hops)):
        await_wave(k)
        if k + 1 < len(hops):
            wave(k + 1)
    nears[seat] = part[:done]
    if inner > 1:
        pltpu.make_async_copy(nears.at[1:], nears.at[1:], precv.at[0]).wait()
    sums = nears[0]
    for j in range(1, inner):
        sums = sums + nears[j]
    fars[bench] = sums
    over(outer, lambda o: far(o).start())
    for g in range(groups):
        take_slow(SWEEPS - 2, g)
        if g + 1 < groups:
            take_fast(SWEEPS - 2, g + 1)
        couple(g)
        correct(SWEEPS - 2, g, True)
    over(n, lambda o: late(o).start())
    lates[me] = part[done:]
    for g in range(groups):
        for k in range(0, rows, STEP):
            at = pl.ds(k, STEP)
            x_out[at, span(g)] = xs[at, span(g)] + (acc[g, at] + zs[g, at]) * scale(at)

    def sent(ref, sem):
        return pltpu.make_async_copy(ref, ref, sem)

    sent(recv.at[:, FAST], send_sem.at[FAST]).wait()

    @pl.when(has)
    def _():
        sent(recv.at[:, SLOW], send_sem.at[SLOW]).wait()
        reflect.wait_send()
    if inner > 1:
        sent(nears.at[1:], psend.at[0]).wait()
    if outer > 1:
        sent(fars.at[1:], psend.at[1]).wait()
        sent(fars.at[1:], precv.at[1]).wait()
    parts = cols // LANES

    def finish(total, first):
        norms = jnp.sqrt(total)
        for s in range(total.shape[0]):
            for g in range(parts):
                norm_out[first + s:first + s + 1, g * LANES:(g + 1) * LANES] = norms[s, g:g + 1]

    finish(sum((fars[j] for j in range(1, outer)), fars[0]), 0)
    lates_all(0).wait()
    lates_all(1).wait()
    terms = [lates[j] for j in range(n)]
    while len(terms) > 1:
        terms = [a + b for a, b in zip(terms[::2], terms[1::2])] + terms[len(terms) // 2 * 2:]
    finish(terms[0], done)


def local(n, diag_blocks, lower_coupling, upper_coupling, right_sides):
    rows, cols = right_sides.shape
    width = lower_coupling.shape[1]
    size = GROUP
    groups, parts = cols // size, cols // LANES
    inner = max(a for a in range(1, n + 1) if n % a == 0 and a * a <= n)
    f32, bf16 = jnp.float32, jnp.bfloat16
    return pl.pallas_call(
        functools.partial(kernel, n),
        out_shape=(pltpu.VMEM((rows, cols), f32), pltpu.VMEM((SWEEPS, cols), f32)),
        in_specs=[pl.BlockSpec(memory_space=pltpu.HBM)] * 4,
        out_specs=[pl.BlockSpec(memory_space=pltpu.VMEM)] * 2,
        scratch_shapes=[
            pltpu.VMEM((rows, rows), f32),
            pltpu.VMEM((2, width, rows), f32),
            pltpu.VMEM((rows, cols), f32),
            pltpu.VMEM((rows, rows), bf16),
            pltpu.VMEM((rows, rows), bf16),
            pltpu.VMEM((rows, 2 * width), f32),
            pltpu.VMEM((rows, 6 * width), bf16),
            pltpu.VMEM((width, 3 * width), bf16),
            pltpu.VMEM((width, 3 * width), bf16),
            pltpu.VMEM((rows, LANES), f32),
            pltpu.VMEM((groups, rows, size), f32),
            pltpu.VMEM((rows, size), bf16),
            pltpu.VMEM((rows, size), bf16),
            pltpu.VMEM((groups, 2, 3 * width, size), bf16),
            pltpu.VMEM((groups, 2, 3 * width, size), bf16),
            pltpu.VMEM((groups, width, size), f32),
            pltpu.VMEM((groups, rows, size), f32),
            pltpu.VMEM((SWEEPS, 2, groups, width, size), f32),
            pltpu.VMEM((SWEEPS - 1, 2, groups, width, size), f32),
            pltpu.VMEM((width // 2, 2 * width), f32),
            pltpu.VMEM((width // 2, 2 * width), f32),
            pltpu.VMEM((SWEEPS, parts, LANES), f32),
            pltpu.VMEM((inner, SWEEPS - 2, parts, LANES), f32),
            pltpu.VMEM((n // inner, SWEEPS - 2, parts, LANES), f32),
            pltpu.VMEM((n, 2, parts, LANES), f32),
            pltpu.SemaphoreType.DMA((rows // LANES + 5,)),
            pltpu.SemaphoreType.DMA((2,)),
            pltpu.SemaphoreType.DMA((SWEEPS - 1, 2, groups)),
            pltpu.SemaphoreType.DMA((2,)),
            pltpu.SemaphoreType.DMA((2,)),
            pltpu.SemaphoreType.DMA((2,)),
            pltpu.SemaphoreType.DMA((2,)),
            pltpu.SemaphoreType.REGULAR((max(len(reaches(n)), 1),)),
        ],
        compiler_params=pltpu.CompilerParams(
            collective_id=0, has_side_effects=True, vmem_limit_bytes=62 * 2**20),
    )(diag_blocks, lower_coupling.T, upper_coupling.T, right_sides)


def solution(mesh):
    return jax.shard_map(
        functools.partial(local, mesh.shape["row"]),
        mesh=mesh,
        in_specs=(P("row", None), P("row", None), P("row", None), P("row", "grp")),
        out_specs=(P("row", "grp"), P(None, "grp")),
        check_vma=False,
    )
```

```python
import functools

import jax
import jax.numpy as jnp
from jax import lax
from jax.experimental import pallas as pl
from jax.experimental.pallas import tpu as pltpu
from jax.sharding import PartitionSpec as P

SWEEPS = 8
LANES = 128
GROUP = 256
STEP = 64
PAUSE = 2


def split(value):
    high = value.astype(jnp.bfloat16)
    low = (value - high.astype(jnp.float32)).astype(jnp.bfloat16)
    return high, low


def dot(left, right):
    return jnp.dot(left, right, preferred_element_type=jnp.float32)


def reaches(n):
    return [hop for hop in (SWEEPS // 2 << k for k in range(n)) if hop < n]


def halves(count):
    return pl.ds(0, count // 2), pl.ds(count // 2, count // 2)


def wide(column, size):
    return column if size == LANES else jnp.concatenate([column] * (size // LANES), axis=1)


def kernel(
    n, d_hbm, l_hbm, u_hbm, b_hbm, x_out, norm_out,
    dv, lu, xs, a_hi, a_lo, cf, c3, cx, w3, inv, acc, hi, lo, halo, own, pre, zs,
    send, recv, gsend, grecv, part, nears, fars, lates, load_sem, send_sem, recv_sem, gsem, psend, precv, lsem, waves,
):
    me = lax.axis_index("row")
    rows, cols = xs.shape
    width = lu.shape[1]
    size = hi.shape[1]
    groups = cols // size
    last = rows - width
    chunks = rows // LANES
    core = lax.rem(me, 2)
    fast_row, slow_row = me + 1 - 2 * core, me - 1 + 2 * core
    has = jnp.logical_and(slow_row >= 0, slow_row < n)
    SLOW, FAST = 0, 1
    slow_rows = pl.ds(pl.multiple_of(core * last, width), width)
    fast_rows = pl.ds(pl.multiple_of((1 - core) * last, width), width)
    rest_rows = [pl.ds(pl.multiple_of(core * width + k * width, width), width) for k in range(last // width)]
    middle = pl.ds(width, last - width)

    order = [core * (chunks - 1), (1 - core) * (chunks - 1)] + list(range(1, chunks - 1))

    def chunk(m):
        return pl.ds(pl.multiple_of(m * LANES, LANES), LANES)

    def load(src, dst, k):
        return pltpu.make_async_copy(src, dst, load_sem.at[k])

    d_loads = [load(d_hbm.at[chunk(m)], dv.at[chunk(m)], k) for k, m in enumerate(order)]
    b_loads = [load(b_hbm.at[r], xs.at[r], chunks + k) for k, r in enumerate((slow_rows, fast_rows, middle))]
    c_loads = [load(l_hbm, lu.at[core], chunks + 3), load(u_hbm, lu.at[1 - core], chunks + 4)]
    edge = pl.ds(pl.multiple_of(core * (rows - LANES), LANES), LANES)
    for copy in (d_loads[0], b_loads[0], *c_loads, d_loads[1], b_loads[1], *d_loads[2:], b_loads[2]):
        copy.start()

    barrier = pltpu.get_barrier_semaphore()

    pl.semaphore_signal(barrier, inc=1, device_id={"row": fast_row})

    @pl.when(has)
    def _():
        pl.semaphore_signal(barrier, inc=1, device_id={"row": slow_row})

    hops = reaches(n)
    reach = SWEEPS // 2

    def wave(k):
        for far_row in (me - hops[k], me + hops[k]):
            @pl.when(jnp.logical_and(far_row >= 0, far_row < n))
            def _():
                pl.semaphore_signal(waves.at[k], inc=1, device_id={"row": far_row})

    def await_wave(k):
        pl.semaphore_wait(waves.at[k], (me >= hops[k]).astype(jnp.int32) + (me + hops[k] < n).astype(jnp.int32))

    @pl.when(jnp.logical_not(has))
    def _():
        recv[:, SLOW] = jnp.zeros_like(recv[:, SLOW])
        grecv[...] = jnp.zeros_like(grecv)

    def copy(s, side, g):
        return pltpu.make_async_remote_copy(
            src_ref=send.at[s, side, g], dst_ref=recv.at[s, side, g],
            send_sem=send_sem.at[side], recv_sem=recv_sem.at[s, side, g],
            device_id={"row": slow_row if side == SLOW else fast_row})

    reflect = pltpu.make_async_remote_copy(
        src_ref=gsend, dst_ref=grecv, send_sem=gsem.at[0], recv_sem=gsem.at[1],
        device_id={"row": slow_row})

    def ship(s, side, g):
        if side == FAST:
            copy(s, side, g).start()
        else:
            @pl.when(has)
            def _():
                copy(s, side, g).start()

    def span(g):
        return slice(g * size, (g + 1) * size)

    def scale(r):
        return wide(inv[r], size)

    def stack(ref, pair, *index):
        for k, value in enumerate((pair[0], pair[1], pair[0])):
            ref[*index, k * width:(k + 1) * width] = value

    def triple(value):
        high, low = split(value)
        return jnp.concatenate([high, high, low], axis=1)

    def keep(r, at, g, s):
        d = r * scale(at)
        hi[at], lo[at] = split(d)
        return d, jnp.sum(r * r, axis=0, keepdims=True)

    def note(s, g, sums):
        per = size // LANES
        for j in range(per):
            part[s, g * per + j:g * per + j + 1] = sums[:, j * LANES:(j + 1) * LANES]

    def advance(g):
        for at in halves(rows):
            total = jnp.zeros((rows // 2, size), jnp.float32)
            for k in halves(rows):
                total = total + (dot(a_hi[at, k], hi[k]) + dot(a_hi[at, k], lo[k]) + dot(a_lo[at, k], hi[k]))
            acc[g, at] = total

    def pivots(m):
        block = dv[chunk(m), chunk(m)]
        eye = (lax.broadcasted_iota(jnp.int32, block.shape, 0)
               == lax.broadcasted_iota(jnp.int32, block.shape, 1))
        pivot = jnp.sum(jnp.where(eye, block, 0.0), axis=1, keepdims=True)
        inv[chunk(m)] = jnp.broadcast_to(1.0 / pivot, block.shape)

    def spread(m):
        for k in range(0, LANES, 32):
            at = pl.ds(pl.multiple_of(m * LANES + k, 32), 32)
            block = dv[at]
            eye = (lax.broadcasted_iota(jnp.int32, block.shape, 0) + (m * LANES + k)
                   == lax.broadcasted_iota(jnp.int32, block.shape, 1))
            a_hi[at], a_lo[at] = split(jnp.where(eye, 0.0, -block))

    d_loads[0].wait()
    pivots(order[0])
    b_loads[0].wait()
    for g in range(groups):
        send[0, SLOW, g] = xs[slow_rows, span(g)] * scale(slow_rows)
    for c_load in c_loads:
        c_load.wait()
    cf[edge] = -jnp.concatenate([lu[0, :, edge], lu[1, :, edge]], axis=0).T
    reflected = cf[slow_rows, :width] * inv[slow_rows, :width]
    gsend[...] = jnp.concatenate([reflected[:width // 2], reflected[width // 2:]], axis=1)
    pl.semaphore_wait(barrier, 1 + has.astype(jnp.int32))
    ship(0, SLOW, 0)
    d_loads[1].wait()
    pivots(order[1])
    b_loads[1].wait()
    for g in range(groups):
        send[0, FAST, g] = xs[fast_rows, span(g)] * scale(fast_rows)
        ship(0, FAST, g)

    cf[...] = -jnp.concatenate([lu[0], lu[1]], axis=0).T
    c3[...] = jnp.concatenate([triple(cf[:, width:]), triple(cf[:, :width])], axis=1)
    cx[...] = triple(cf[slow_rows, width:])
    for m in order[:2]:
        spread(m)
    for k, m in enumerate(order[2:]):
        d_loads[2 + k].wait()
        pivots(m)
        spread(m)

    b_loads[2].wait()
    for g in range(groups):
        total = jnp.zeros((1, size), jnp.float32)
        for k in range(0, rows, STEP):
            at = pl.ds(k, STEP)
            d, sums = keep(xs[at, span(g)], at, g, 0)
            total = total + sums
            xs[at, span(g)] = d
        note(0, g, total)
        stack(own, (hi[slow_rows], lo[slow_rows]), g, 0)
        pre[g] = jnp.zeros_like(pre[g])
        advance(g)
        if g + 1 < groups:
            ship(0, SLOW, g + 1)

    @pl.when(has)
    def _():
        reflect.start()

    def share(g):
        return dot(cx[...], halo[g, 0].reshape(3 * width, size))

    def early(s, g, z):
        send[s + 1, SLOW, g] = (acc[g, slow_rows] + z) * scale(slow_rows)

        @pl.when(jnp.logical_and(has, s < SWEEPS - 2))
        def _():
            copy(s + 1, SLOW, g).start()

    def take_fast(s, g):
        copy(s, FAST, g).wait_recv()
        stack(halo, split(recv[s, FAST, g]), g, 0)

    def take_slow(s, g):
        @pl.when(has)
        def _():
            copy(s, SLOW, g).wait_recv()
        stack(halo, split(recv[s, SLOW, g] + pre[g]), g, 1)

    def correct(s, g, final, between=lambda: None):
        total = jnp.zeros((1, size), jnp.float32)
        for k, at in enumerate((fast_rows, *rest_rows)):
            if k == PAUSE:
                between()
            r = acc[g, at] + zs[g, at]
            if final:
                total = total + jnp.sum(r * r, axis=0, keepdims=True)
                continue
            d, sums = keep(r, at, g, s + 1)
            total = total + sums
            if at is fast_rows:
                send[s + 1, FAST, g] = d
                ship(s + 1, FAST, g)
            xs[at, span(g)] += d
        note(s + 1, g, total)

    def couple(g):
        for at in halves(rows):
            zs[g, at] = dot(c3[at], halo[g].reshape(6 * width, size))

    take_fast(0, 0)
    early(0, 0, share(0))

    inner = nears.shape[0]
    outer = n // inner
    seat, bench = lax.rem(me, inner), lax.div(me, inner)
    done = SWEEPS - 2

    def near(o):
        return pltpu.make_async_remote_copy(
            src_ref=part.at[:done], dst_ref=nears.at[seat],
            send_sem=psend.at[0], recv_sem=precv.at[0],
            device_id={"row": bench * inner + lax.rem(seat + o, inner)})

    def far(o):
        return pltpu.make_async_remote_copy(
            src_ref=fars.at[bench], dst_ref=fars.at[bench],
            send_sem=psend.at[1], recv_sem=precv.at[1],
            device_id={"row": lax.rem(bench + o, outer) * inner + seat})

    def late(o):
        return pltpu.make_async_remote_copy(
            src_ref=part.at[done:], dst_ref=lates.at[me],
            send_sem=lsem.at[0], recv_sem=lsem.at[1],
            device_id={"row": lax.rem(me + o, n)})

    def lates_all(k):
        return pltpu.make_async_copy(lates.at[1:], lates.at[1:], lsem.at[k])

    def over(count, action):
        def one(o, carry):
            action(o)
            return carry

        lax.fori_loop(1, count, one, 0)

    def step(s, g, known):
        ahead = (s, g + 1) if g + 1 < groups else (s + 1, 0)
        take_slow(s, g)
        couple(g)
        take_fast(*ahead)
        z = share(ahead[1])
        if known:
            pre[g] = dot(w3[...], own[g, 1])
        correct(s, g, False, lambda: early(*ahead, z))
        advance(g)
        stack(own, (hi[slow_rows], lo[slow_rows]), g, 1)

    for g in range(groups):
        step(0, g, False)

    @pl.when(has)
    def _():
        reflect.wait_recv()
    gathered = grecv[...]
    w3[...] = triple(jnp.concatenate([gathered[:, :width], gathered[:, width:]], axis=0))
    for g in range(groups):
        pre[g] = dot(w3[...], own[g, 0])
    def body(s, carry):
        if hops:
            @pl.when(s == reach - 1)
            def _():
                wave(0)

        @pl.when(s == SWEEPS - 3)
        def _():
            if hops:
                await_wave(0)
            if len(hops) > 1:
                wave(1)
            over(inner, lambda o: near(o).start())
        for g in range(groups):
            step(s, g, True)
        return carry

    lax.fori_loop(1, SWEEPS - 2, body, 0)
    for k in range(1, len(hops)):
        await_wave(k)
        if k + 1 < len(hops):
            wave(k + 1)
    nears[seat] = part[:done]
    if inner > 1:
        pltpu.make_async_copy(nears.at[1:], nears.at[1:], precv.at[0]).wait()
    sums = nears[0]
    for j in range(1, inner):
        sums = sums + nears[j]
    fars[bench] = sums
    over(outer, lambda o: far(o).start())
    for g in range(groups):
        take_slow(SWEEPS - 2, g)
        if g + 1 < groups:
            take_fast(SWEEPS - 2, g + 1)
        couple(g)
        correct(SWEEPS - 2, g, True)
    for o in range(1, n):
        late(o).start()
    lates[me] = part[done:]
    for g in range(groups):
        for k in range(0, rows, STEP):
            at = pl.ds(k, STEP)
            x_out[at, span(g)] = xs[at, span(g)] + (acc[g, at] + zs[g, at]) * scale(at)

    def sent(ref, sem):
        return pltpu.make_async_copy(ref, ref, sem)

    sent(recv.at[:, FAST], send_sem.at[FAST]).wait()

    @pl.when(has)
    def _():
        sent(recv.at[:, SLOW], send_sem.at[SLOW]).wait()
        reflect.wait_send()
    if inner > 1:
        sent(nears.at[1:], psend.at[0]).wait()
    if outer > 1:
        sent(fars.at[1:], psend.at[1]).wait()
        sent(fars.at[1:], precv.at[1]).wait()
    parts = cols // LANES

    def finish(total, first):
        norms = jnp.sqrt(total)
        for s in range(total.shape[0]):
            for g in range(parts):
                norm_out[first + s:first + s + 1, g * LANES:(g + 1) * LANES] = norms[s, g:g + 1]

    finish(sum((fars[j] for j in range(1, outer)), fars[0]), 0)
    lates_all(0).wait()
    lates_all(1).wait()
    terms = [lates[j] for j in range(n)]
    while len(terms) > 1:
        terms = [a + b for a, b in zip(terms[::2], terms[1::2])] + terms[len(terms) // 2 * 2:]
    finish(terms[0], done)


def local(n, diag_blocks, lower_coupling, upper_coupling, right_sides):
    rows, cols = right_sides.shape
    width = lower_coupling.shape[1]
    size = GROUP
    groups, parts = cols // size, cols // LANES
    inner = max(a for a in range(1, n + 1) if n % a == 0 and a * a <= n)
    f32, bf16 = jnp.float32, jnp.bfloat16
    return pl.pallas_call(
        functools.partial(kernel, n),
        out_shape=(pltpu.VMEM((rows, cols), f32), pltpu.VMEM((SWEEPS, cols), f32)),
        in_specs=[pl.BlockSpec(memory_space=pltpu.HBM)] * 4,
        out_specs=[pl.BlockSpec(memory_space=pltpu.VMEM)] * 2,
        scratch_shapes=[
            pltpu.VMEM((rows, rows), f32),
            pltpu.VMEM((2, width, rows), f32),
            pltpu.VMEM((rows, cols), f32),
            pltpu.VMEM((rows, rows), bf16),
            pltpu.VMEM((rows, rows), bf16),
            pltpu.VMEM((rows, 2 * width), f32),
            pltpu.VMEM((rows, 6 * width), bf16),
            pltpu.VMEM((width, 3 * width), bf16),
            pltpu.VMEM((width, 3 * width), bf16),
            pltpu.VMEM((rows, LANES), f32),
            pltpu.VMEM((groups, rows, size), f32),
            pltpu.VMEM((rows, size), bf16),
            pltpu.VMEM((rows, size), bf16),
            pltpu.VMEM((groups, 2, 3 * width, size), bf16),
            pltpu.VMEM((groups, 2, 3 * width, size), bf16),
            pltpu.VMEM((groups, width, size), f32),
            pltpu.VMEM((groups, rows, size), f32),
            pltpu.VMEM((SWEEPS, 2, groups, width, size), f32),
            pltpu.VMEM((SWEEPS - 1, 2, groups, width, size), f32),
            pltpu.VMEM((width // 2, 2 * width), f32),
            pltpu.VMEM((width // 2, 2 * width), f32),
            pltpu.VMEM((SWEEPS, parts, LANES), f32),
            pltpu.VMEM((inner, SWEEPS - 2, parts, LANES), f32),
            pltpu.VMEM((n // inner, SWEEPS - 2, parts, LANES), f32),
            pltpu.VMEM((n, 2, parts, LANES), f32),
            pltpu.SemaphoreType.DMA((rows // LANES + 5,)),
            pltpu.SemaphoreType.DMA((2,)),
            pltpu.SemaphoreType.DMA((SWEEPS - 1, 2, groups)),
            pltpu.SemaphoreType.DMA((2,)),
            pltpu.SemaphoreType.DMA((2,)),
            pltpu.SemaphoreType.DMA((2,)),
            pltpu.SemaphoreType.DMA((2,)),
            pltpu.SemaphoreType.REGULAR((max(len(reaches(n)), 1),)),
        ],
        compiler_params=pltpu.CompilerParams(
            collective_id=0, has_side_effects=True, vmem_limit_bytes=62 * 2**20),
    )(diag_blocks, lower_coupling.T, upper_coupling.T, right_sides)


def solution(mesh):
    return jax.shard_map(
        functools.partial(local, mesh.shape["row"]),
        mesh=mesh,
        in_specs=(P("row", None), P("row", None), P("row", None), P("row", "grp")),
        out_specs=(P("row", "grp"), P(None, "grp")),
        check_vma=False,
    )
```

```python
import functools

import jax
import jax.numpy as jnp
from jax import lax
from jax.experimental import pallas as pl
from jax.experimental.pallas import tpu as pltpu
from jax.sharding import PartitionSpec as P

SWEEPS = 8
LANES = 128
GROUP = 256
STEP = 64
PAUSE = 2


def split(value):
    high = value.astype(jnp.bfloat16)
    low = (value - high.astype(jnp.float32)).astype(jnp.bfloat16)
    return high, low


def dot(left, right):
    return jnp.dot(left, right, preferred_element_type=jnp.float32)


def reaches(n):
    return [hop for hop in (SWEEPS // 2 << k for k in range(n)) if hop < n]


def halves(count):
    return pl.ds(0, count // 2), pl.ds(count // 2, count // 2)


def wide(column, size):
    return column if size == LANES else jnp.concatenate([column] * (size // LANES), axis=1)


def kernel(
    n, d_hbm, l_hbm, u_hbm, b_hbm, x_out, norm_out,
    dv, lu, xs, a_hi, a_lo, cf, c3, cx, w3, inv, acc, hi, lo, halo, own, pre, zs,
    send, recv, gsend, grecv, part, nears, fars, lates, load_sem, send_sem, recv_sem, gsem, psend, precv, lsem, waves,
):
    me = lax.axis_index("row")
    rows, cols = xs.shape
    width = lu.shape[1]
    size = hi.shape[1]
    groups = cols // size
    last = rows - width
    chunks = rows // LANES
    core = lax.rem(me, 2)
    fast_row, slow_row = me + 1 - 2 * core, me - 1 + 2 * core
    has = jnp.logical_and(slow_row >= 0, slow_row < n)
    SLOW, FAST = 0, 1
    slow_rows = pl.ds(pl.multiple_of(core * last, width), width)
    fast_rows = pl.ds(pl.multiple_of((1 - core) * last, width), width)
    rest_rows = [pl.ds(pl.multiple_of(core * width + k * width, width), width) for k in range(last // width)]
    middle = pl.ds(width, last - width)

    order = [core * (chunks - 1), (1 - core) * (chunks - 1)] + list(range(1, chunks - 1))

    def chunk(m):
        return pl.ds(pl.multiple_of(m * LANES, LANES), LANES)

    def load(src, dst, k):
        return pltpu.make_async_copy(src, dst, load_sem.at[k])

    d_loads = [load(d_hbm.at[chunk(m)], dv.at[chunk(m)], k) for k, m in enumerate(order)]
    b_loads = [load(b_hbm.at[r], xs.at[r], chunks + k) for k, r in enumerate((slow_rows, fast_rows, middle))]
    c_loads = [load(l_hbm, lu.at[core], chunks + 3), load(u_hbm, lu.at[1 - core], chunks + 3)]
    edge = pl.ds(pl.multiple_of(core * (rows - LANES), LANES), LANES)
    for copy in (d_loads[0], b_loads[0], *c_loads, d_loads[1], b_loads[1], *d_loads[2:], b_loads[2]):
        copy.start()

    barrier = pltpu.get_barrier_semaphore()

    pl.semaphore_signal(barrier, inc=1, device_id={"row": fast_row})

    @pl.when(has)
    def _():
        pl.semaphore_signal(barrier, inc=1, device_id={"row": slow_row})

    hops = reaches(n)
    reach = SWEEPS // 2

    def wave(k):
        for far_row in (me - hops[k], me + hops[k]):
            @pl.when(jnp.logical_and(far_row >= 0, far_row < n))
            def _():
                pl.semaphore_signal(waves.at[k], inc=1, device_id={"row": far_row})

    def await_wave(k):
        pl.semaphore_wait(waves.at[k], (me >= hops[k]).astype(jnp.int32) + (me + hops[k] < n).astype(jnp.int32))

    @pl.when(jnp.logical_not(has))
    def _():
        recv[:, SLOW] = jnp.zeros_like(recv[:, SLOW])
        grecv[...] = jnp.zeros_like(grecv)

    def copy(s, side, g):
        return pltpu.make_async_remote_copy(
            src_ref=send.at[s, side, g], dst_ref=recv.at[s, side, g],
            send_sem=send_sem.at[side], recv_sem=recv_sem.at[s, side, g],
            device_id={"row": slow_row if side == SLOW else fast_row})

    reflect = pltpu.make_async_remote_copy(
        src_ref=gsend, dst_ref=grecv, send_sem=gsem.at[0], recv_sem=gsem.at[1],
        device_id={"row": slow_row})

    def ship(s, side, g):
        if side == FAST:
            copy(s, side, g).start()
        else:
            @pl.when(has)
            def _():
                copy(s, side, g).start()

    def span(g):
        return slice(g * size, (g + 1) * size)

    def scale(r):
        return wide(inv[r], size)

    def stack(ref, pair, *index):
        for k, value in enumerate((pair[0], pair[1], pair[0])):
            ref[*index, k * width:(k + 1) * width] = value

    def triple(value):
        high, low = split(value)
        return jnp.concatenate([high, high, low], axis=1)

    def keep(r, at, g, s):
        d = r * scale(at)
        hi[at], lo[at] = split(d)
        return d, jnp.sum(r * r, axis=0, keepdims=True)

    def note(s, g, sums):
        per = size // LANES
        for j in range(per):
            part[s, g * per + j:g * per + j + 1] = sums[:, j * LANES:(j + 1) * LANES]

    def advance(g):
        for at in halves(rows):
            total = jnp.zeros((rows // 2, size), jnp.float32)
            for k in halves(rows):
                total = total + (dot(a_hi[at, k], hi[k]) + dot(a_hi[at, k], lo[k]) + dot(a_lo[at, k], hi[k]))
            acc[g, at] = total

    def pivots(m):
        block = dv[chunk(m), chunk(m)]
        eye = (lax.broadcasted_iota(jnp.int32, block.shape, 0)
               == lax.broadcasted_iota(jnp.int32, block.shape, 1))
        pivot = jnp.sum(jnp.where(eye, block, 0.0), axis=1, keepdims=True)
        inv[chunk(m)] = jnp.broadcast_to(1.0 / pivot, block.shape)

    def spread(m):
        for k in range(0, LANES, 32):
            at = pl.ds(pl.multiple_of(m * LANES + k, 32), 32)
            block = dv[at]
            eye = (lax.broadcasted_iota(jnp.int32, block.shape, 0) + (m * LANES + k)
                   == lax.broadcasted_iota(jnp.int32, block.shape, 1))
            a_hi[at], a_lo[at] = split(jnp.where(eye, 0.0, -block))

    d_loads[0].wait()
    pivots(order[0])
    b_loads[0].wait()
    for g in range(groups):
        send[0, SLOW, g] = xs[slow_rows, span(g)] * scale(slow_rows)
    load(lu, lu, chunks + 3).wait()
    cf[edge] = -jnp.concatenate([lu[0, :, edge], lu[1, :, edge]], axis=0).T
    reflected = cf[slow_rows, :width] * inv[slow_rows, :width]
    gsend[...] = jnp.concatenate([reflected[:width // 2], reflected[width // 2:]], axis=1)
    pl.semaphore_wait(barrier, 1 + has.astype(jnp.int32))
    ship(0, SLOW, 0)
    d_loads[1].wait()
    pivots(order[1])
    b_loads[1].wait()
    for g in range(groups):
        send[0, FAST, g] = xs[fast_rows, span(g)] * scale(fast_rows)
        ship(0, FAST, g)

    cf[...] = -jnp.concatenate([lu[0], lu[1]], axis=0).T
    c3[...] = jnp.concatenate([triple(cf[:, width:]), triple(cf[:, :width])], axis=1)
    cx[...] = triple(cf[slow_rows, width:])
    for m in order[:2]:
        spread(m)
    for k, m in enumerate(order[2:]):
        d_loads[2 + k].wait()
        pivots(m)
        spread(m)

    b_loads[2].wait()
    for g in range(groups):
        total = jnp.zeros((1, size), jnp.float32)
        for k in range(0, rows, STEP):
            at = pl.ds(k, STEP)
            d, sums = keep(xs[at, span(g)], at, g, 0)
            total = total + sums
            xs[at, span(g)] = d
        note(0, g, total)
        stack(own, (hi[slow_rows], lo[slow_rows]), g, 0)
        pre[g] = jnp.zeros_like(pre[g])
        advance(g)
        if g + 1 < groups:
            ship(0, SLOW, g + 1)

    @pl.when(has)
    def _():
        reflect.start()

    def share(g):
        return dot(cx[...], halo[g, 0].reshape(3 * width, size))

    def early(s, g, z):
        send[s + 1, SLOW, g] = (acc[g, slow_rows] + z) * scale(slow_rows)

        @pl.when(jnp.logical_and(has, s < SWEEPS - 2))
        def _():
            copy(s + 1, SLOW, g).start()

    def take_fast(s, g):
        copy(s, FAST, g).wait_recv()
        stack(halo, split(recv[s, FAST, g]), g, 0)

    def take_slow(s, g):
        @pl.when(has)
        def _():
            copy(s, SLOW, g).wait_recv()
        stack(halo, split(recv[s, SLOW, g] + pre[g]), g, 1)

    def correct(s, g, final, between=lambda: None):
        total = jnp.zeros((1, size), jnp.float32)
        for k, at in enumerate((fast_rows, *rest_rows)):
            if k == PAUSE:
                between()
            r = acc[g, at] + zs[g, at]
            if final:
                total = total + jnp.sum(r * r, axis=0, keepdims=True)
                continue
            d, sums = keep(r, at, g, s + 1)
            total = total + sums
            if at is fast_rows:
                send[s + 1, FAST, g] = d
                ship(s + 1, FAST, g)
            xs[at, span(g)] += d
        note(s + 1, g, total)

    def couple(g):
        for at in halves(rows):
            zs[g, at] = dot(c3[at], halo[g].reshape(6 * width, size))

    take_fast(0, 0)
    early(0, 0, share(0))

    inner = nears.shape[0]
    outer = n // inner
    seat, bench = lax.rem(me, inner), lax.div(me, inner)
    done = SWEEPS - 2

    def near(o):
        return pltpu.make_async_remote_copy(
            src_ref=part.at[:done], dst_ref=nears.at[seat],
            send_sem=psend.at[0], recv_sem=precv.at[0],
            device_id={"row": bench * inner + lax.rem(seat + o, inner)})

    def far(o):
        return pltpu.make_async_remote_copy(
            src_ref=fars.at[bench], dst_ref=fars.at[bench],
            send_sem=psend.at[1], recv_sem=precv.at[1],
            device_id={"row": lax.rem(bench + o, outer) * inner + seat})

    def late(o):
        return pltpu.make_async_remote_copy(
            src_ref=part.at[done:], dst_ref=lates.at[me],
            send_sem=lsem.at[0], recv_sem=lsem.at[1],
            device_id={"row": lax.rem(me + o, n)})

    def lates_all(k):
        return pltpu.make_async_copy(lates.at[1:], lates.at[1:], lsem.at[k])

    def over(count, action):
        def one(o, carry):
            action(o)
            return carry

        lax.fori_loop(1, count, one, 0)

    def step(s, g, known):
        ahead = (s, g + 1) if g + 1 < groups else (s + 1, 0)
        take_slow(s, g)
        couple(g)
        take_fast(*ahead)
        z = share(ahead[1])
        if known:
            pre[g] = dot(w3[...], own[g, 1])
        correct(s, g, False, lambda: early(*ahead, z))
        advance(g)
        stack(own, (hi[slow_rows], lo[slow_rows]), g, 1)

    for g in range(groups):
        step(0, g, False)

    @pl.when(has)
    def _():
        reflect.wait_recv()
    gathered = grecv[...]
    w3[...] = triple(jnp.concatenate([gathered[:, :width], gathered[:, width:]], axis=0))
    for g in range(groups):
        pre[g] = dot(w3[...], own[g, 0])
    def body(s, carry):
        if hops:
            @pl.when(s == reach - 1)
            def _():
                wave(0)

        @pl.when(s == SWEEPS - 3)
        def _():
            if hops:
                await_wave(0)
            if len(hops) > 1:
                wave(1)
            over(inner, lambda o: near(o).start())
        for g in range(groups):
            step(s, g, True)
        return carry

    lax.fori_loop(1, SWEEPS - 2, body, 0)
    for k in range(1, len(hops)):
        await_wave(k)
        if k + 1 < len(hops):
            wave(k + 1)
    nears[seat] = part[:done]
    if inner > 1:
        pltpu.make_async_copy(nears.at[1:], nears.at[1:], precv.at[0]).wait()
    sums = nears[0]
    for j in range(1, inner):
        sums = sums + nears[j]
    fars[bench] = sums
    over(outer, lambda o: far(o).start())
    for g in range(groups):
        take_slow(SWEEPS - 2, g)
        if g + 1 < groups:
            take_fast(SWEEPS - 2, g + 1)
        couple(g)
        correct(SWEEPS - 2, g, True)
    for o in range(1, n):
        late(o).start()
    lates[me] = part[done:]
    for g in range(groups):
        for k in range(0, rows, STEP):
            at = pl.ds(k, STEP)
            x_out[at, span(g)] = xs[at, span(g)] + (acc[g, at] + zs[g, at]) * scale(at)

    def sent(ref, sem):
        return pltpu.make_async_copy(ref, ref, sem)

    sent(recv.at[:, FAST], send_sem.at[FAST]).wait()

    @pl.when(has)
    def _():
        sent(recv.at[:, SLOW], send_sem.at[SLOW]).wait()
        reflect.wait_send()
    if inner > 1:
        sent(nears.at[1:], psend.at[0]).wait()
    if outer > 1:
        sent(fars.at[1:], psend.at[1]).wait()
        sent(fars.at[1:], precv.at[1]).wait()
    parts = cols // LANES

    def finish(total, first):
        norms = jnp.sqrt(total)
        for s in range(total.shape[0]):
            for g in range(parts):
                norm_out[first + s:first + s + 1, g * LANES:(g + 1) * LANES] = norms[s, g:g + 1]

    finish(sum((fars[j] for j in range(1, outer)), fars[0]), 0)
    lates_all(0).wait()
    lates_all(1).wait()
    terms = [lates[j] for j in range(n)]
    while len(terms) > 1:
        terms = [a + b for a, b in zip(terms[::2], terms[1::2])] + terms[len(terms) // 2 * 2:]
    finish(terms[0], done)


def local(n, diag_blocks, lower_coupling, upper_coupling, right_sides):
    rows, cols = right_sides.shape
    width = lower_coupling.shape[1]
    size = GROUP
    groups, parts = cols // size, cols // LANES
    inner = max(a for a in range(1, n + 1) if n % a == 0 and a * a <= n)
    f32, bf16 = jnp.float32, jnp.bfloat16
    return pl.pallas_call(
        functools.partial(kernel, n),
        out_shape=(pltpu.VMEM((rows, cols), f32), pltpu.VMEM((SWEEPS, cols), f32)),
        in_specs=[pl.BlockSpec(memory_space=pltpu.HBM)] * 4,
        out_specs=[pl.BlockSpec(memory_space=pltpu.VMEM)] * 2,
        scratch_shapes=[
            pltpu.VMEM((rows, rows), f32),
            pltpu.VMEM((2, width, rows), f32),
            pltpu.VMEM((rows, cols), f32),
            pltpu.VMEM((rows, rows), bf16),
            pltpu.VMEM((rows, rows), bf16),
            pltpu.VMEM((rows, 2 * width), f32),
            pltpu.VMEM((rows, 6 * width), bf16),
            pltpu.VMEM((width, 3 * width), bf16),
            pltpu.VMEM((width, 3 * width), bf16),
            pltpu.VMEM((rows, LANES), f32),
            pltpu.VMEM((groups, rows, size), f32),
            pltpu.VMEM((rows, size), bf16),
            pltpu.VMEM((rows, size), bf16),
            pltpu.VMEM((groups, 2, 3 * width, size), bf16),
            pltpu.VMEM((groups, 2, 3 * width, size), bf16),
            pltpu.VMEM((groups, width, size), f32),
            pltpu.VMEM((groups, rows, size), f32),
            pltpu.VMEM((SWEEPS, 2, groups, width, size), f32),
            pltpu.VMEM((SWEEPS - 1, 2, groups, width, size), f32),
            pltpu.VMEM((width // 2, 2 * width), f32),
            pltpu.VMEM((width // 2, 2 * width), f32),
            pltpu.VMEM((SWEEPS, parts, LANES), f32),
            pltpu.VMEM((inner, SWEEPS - 2, parts, LANES), f32),
            pltpu.VMEM((n // inner, SWEEPS - 2, parts, LANES), f32),
            pltpu.VMEM((n, 2, parts, LANES), f32),
            pltpu.SemaphoreType.DMA((rows // LANES + 4,)),
            pltpu.SemaphoreType.DMA((2,)),
            pltpu.SemaphoreType.DMA((SWEEPS - 1, 2, groups)),
            pltpu.SemaphoreType.DMA((2,)),
            pltpu.SemaphoreType.DMA((2,)),
            pltpu.SemaphoreType.DMA((2,)),
            pltpu.SemaphoreType.DMA((2,)),
            pltpu.SemaphoreType.REGULAR((max(len(reaches(n)), 1),)),
        ],
        compiler_params=pltpu.CompilerParams(
            collective_id=0, has_side_effects=True, vmem_limit_bytes=62 * 2**20),
    )(diag_blocks, lower_coupling.T, upper_coupling.T, right_sides)


def solution(mesh):
    return jax.shard_map(
        functools.partial(local, mesh.shape["row"]),
        mesh=mesh,
        in_specs=(P("row", None), P("row", None), P("row", None), P("row", "grp")),
        out_specs=(P("row", "grp"), P(None, "grp")),
        check_vma=False,
    )
```
